256 devices in a mesh: blk: 128 (over x, z, y), row: 2 (over core).
Axes of the slice: x: 4, y: 4, z: 8, core: 2. Of those that a mesh axis runs over, the one named last changes fastest.
Arguments:
- genotypes: bfloat16 [1024, 128, 2048], P('blk', None, 'row'), may hold values from 0 to 2
- assignment: int32 [128], replicated, may hold values from 0 to 127, each once
- snp_counts: int32 [128], replicated, may hold values from 1024 to 2048, as said below
- basis: float32 [128, 64, 2048], P('blk', None, 'row'), may hold values from -6 to 6
Outputs:
- image: float32 [128, 64, 2048], P('blk', None, 'row')
- new_basis: float32 [128, 64, 2048], P('blk', None, 'row')
- factor: float32 [128, 64, 64], P('blk')
The draws below stay inside these ranges and needn't reach their ends.
Inputs may be any that keep to these rules, and one draw needn't show every extreme that they name: `assignment`: each block number appears exactly once. `snp_counts`: A block's SNPs fill its leading slots.
All inputs are finite; a program needn't handle non-finite values.
Results may differ from the reference program's by a relative error of at most 0.0021.
Values may be sent and summed in bfloat16 or wider, within the bound.
A program may use at most 64 MiB of HBM per device.

```python
import jax
import jax.numpy as jnp
from jax import lax

BS = 2048
RANK = 64
SAMPLES = 1024
BLOCKS = 128


def draw_snp_counts(key, part):
    return jax.random.randint(key, (BLOCKS,), BS // 2, BS + 1).astype(jnp.int32)


def level_of(rng, shape, cuts, least, top_value):
    factor_of, own = 1.0, jax.random.fold_in(rng, 6)
    for dim, shards_of in cuts:
        steps = jnp.exp(jax.random.uniform(jax.random.fold_in(own, dim), (shards_of,), jnp.float32, least / len(cuts), top_value / len(cuts)))
        factor_of = factor_of * jnp.repeat(steps, shape[dim] // shards_of).reshape([-1 if axis == dim else 1 for axis in range(len(shape))])
    return factor_of


def bell_draw(rng, dims, width, bound, split=(), held_as=jnp.bfloat16):
    values = width * jax.random.normal(rng, dims, jnp.float32)
    if split:
        values = values * level_of(rng, dims, split, -0.22, 0.18)
    return jnp.clip(values, -bound, bound).astype(held_as)


def setup_inputs(seed: int = 0) -> dict:
    seeds = jax.random.split(jax.random.key(seed), 5)
    genotypes = jnp.clip(2.0 * jax.random.uniform(seeds[0], (SAMPLES, BLOCKS, BS), jnp.float32) ** level_of(seeds[0], (SAMPLES, BLOCKS, BS), ((0, 128), (2, 2)), -0.2, 0.2), 0.0, 2.0).astype(jnp.bfloat16)
    assignment = jax.random.permutation(seeds[1], BLOCKS).astype(jnp.int32)
    snp_counts = draw_snp_counts(jax.random.fold_in(seeds[4], 71), 0)
    basis = bell_draw(seeds[3], (BLOCKS, RANK, BS), 1.0, 6.0, ((0, 128), (2, 2)), jnp.float32)
    return {"genotypes": genotypes, "assignment": assignment, "snp_counts": snp_counts, "basis": basis}


epsilon = 1e-05
shrink_weight = 0.5

def reference(genotypes, assignment, snp_counts, basis):
    positions = jnp.arange(BS, dtype=jnp.int32)

    def per_slot(slot_idx):
        block_id = assignment[slot_idx]
        dosage = lax.dynamic_index_in_dim(genotypes, block_id, 1, keepdims=False).astype(jnp.float32)
        live_mask = positions < snp_counts[block_id]
        col_mean = lax.optimization_barrier(jnp.mean(dosage, axis=0))
        centered = dosage - col_mean[None, :]
        col_var = lax.optimization_barrier(jnp.mean(centered * centered, axis=0))
        standard = jnp.where(live_mask[None, :], centered * lax.rsqrt(col_var + epsilon)[None, :], 0.0).astype(jnp.bfloat16)
        standard_f = standard.astype(jnp.float32)
        start_basis = basis[slot_idx]
        projected = jnp.dot(standard_f, start_basis.T, precision=lax.Precision.HIGHEST)
        product = jnp.dot(projected.T, standard_f, precision=lax.Precision.HIGHEST) / SAMPLES
        image = shrink_weight * product + (1.0 - shrink_weight) * jnp.where(live_mask[None, :], start_basis, 0.0)
        gram_sum = jnp.dot(image, image.T, precision=lax.Precision.HIGHEST)
        factor = jnp.linalg.cholesky(gram_sum)
        new_basis = jax.scipy.linalg.solve_triangular(factor, image, lower=True)
        return (image, new_basis, factor)
    image, new_basis, factor = lax.map(per_slot, jnp.arange(BLOCKS, dtype=jnp.int32))
    return (image, new_basis, factor)
```

```python
import functools

import jax
import jax.numpy as jnp
from jax import lax
from jax.experimental import pallas as pl
from jax.experimental.pallas import tpu as pltpu
from jax.sharding import PartitionSpec as P

EPS = 1e-05
SHRINK = 0.5
MESH = pl.DeviceIdType.MESH
NX, NZ, NY = 4, 8, 4
PLANE = NX * NY
BLOCKS = NX * NZ * NY
OWN = 8
SAMPLES = BLOCKS * OWN
HALF = 1024
RANK = 64
CHUNK = 256
KX = (1, 2, 3, 0)
PAIRS = ((1, 7), (4,), (2, 6), (3, 5))
BF = jnp.bfloat16
F32 = jnp.float32


def block_of(x, z, y):
    return (x * NZ + z) * NY + y


def remote(src, dst, send_sem, recv_sem, to):
    return pltpu.make_async_remote_copy(
        src_ref=src, dst_ref=dst, send_sem=send_sem, recv_sem=recv_sem,
        device_id=to, device_id_type=MESH,
    )


def split(value):
    high = value.astype(BF)
    low = (value - high.astype(F32)).astype(BF)
    return jnp.concatenate([high, low], axis=0)


def nt(a, b):
    return lax.dot_general(a, b, (((1,), (1,)), ((), ())), preferred_element_type=F32)


def nn(a, b):
    return lax.dot_general(a, b, (((1,), (0,)), ((), ())), preferred_element_type=F32)


def exchange_kernel(
    assign, counts, geno, basis, image_out, gram_out,
    pick, send, zbuf, fin, std, bsplit, pbuf, precv, gbuf, grecv,
    zss, fss, pss, gss, zrs, grs, prs, grr,
):
    me = lax.axis_index("blk")
    row = lax.axis_index("row")
    y = me % NY
    z = (me // NY) % NZ
    x = me // (NY * NZ)
    mate = {"row": 1 - row}
    here = {"blk": me}

    barrier = pltpu.get_barrier_semaphore()
    xs = [(x + k) % NX for k in range(NX)]
    ys = [(y + k) % NY for k in range(NY)]
    peers = [{"blk": block_of(x, (z + d) % NZ, y)} for d in range(1, NZ)]
    peers += [
        {"blk": block_of(xs[i], z, ys[j])} for i in range(NX) for j in range(NY) if i or j
    ]
    peers.append(mate)
    for peer in peers:
        pl.semaphore_signal(barrier, inc=1, device_id=peer, device_id_type=MESH)

    bsplit[...] = split(basis[...])
    gbuf[...] = jnp.zeros_like(gbuf)
    offset = (
        lax.broadcasted_iota(jnp.int32, (OWN, SAMPLES), 1)
        - BLOCKS * lax.broadcasted_iota(jnp.int32, (OWN, SAMPLES), 0)
    )

    def permute(dz):
        zt = (z + dz) % NZ
        for i in range(NX):
            for j in range(NY):
                slot = block_of(xs[KX[i]], zt, j)
                pick[pl.ds((i * NY + j) * OWN, OWN), :] = jnp.where(
                    offset == assign[slot], 1.0, 0.0
                ).astype(BF)
        table = geno[...].reshape(SAMPLES, HALF)
        moved = nn(pick[...], table).astype(BF).reshape(NX, NY, OWN, HALF)
        for i in range(NX):
            send[pl.ds(block_of(xs[KX[i]], zt, 0), NY)] = moved[i]

    def forward(dz, kx):
        for ky in range(NY):
            if kx == 0 and ky == 0:
                continue
            to = block_of(xs[kx], z, ys[ky])
            src = send.at[to] if dz == 0 else zbuf.at[dz, xs[kx], ys[ky]]
            remote(src, fin.at[dz, kx * NY + ky], fss, grs.at[dz], {"blk": to}).start()

    def zsend(dz):
        zt = (z + dz) % NZ
        to = {"blk": block_of(x, zt, y)}
        for kx in KX[:3]:
            remote(
                send.at[pl.ds(block_of(xs[kx], zt, 0), NY)], zbuf.at[dz, xs[kx]],
                zss, zrs.at[dz, kx], to,
            ).start()
        for ky in (1, 2, 3):
            remote(
                send.at[block_of(x, zt, ys[ky])], zbuf.at[dz, x, ys[ky]],
                zss, zrs.at[dz, 0], to,
            ).start()
        remote(send.at[block_of(x, zt, y)], fin.at[dz, 0], zss, grs.at[dz], to).start()

    def wait_z(dz, kx):
        part = zbuf.at[dz, 0, pl.ds(0, 3)] if kx == 0 else zbuf.at[dz, 0]
        remote(part, part, zss, zrs.at[dz, kx], here).wait_recv()

    for step, dz in enumerate((1, 7, 0, 4, 2, 6, 3, 5)):
        permute(dz)
        if step == 0:
            pl.semaphore_wait(barrier, len(peers))
        if dz == 0:
            for kx in KX:
                forward(0, kx)
            fin[0, 0] = send[me]
        else:
            zsend(dz)

    def wait_group(dz):
        part = fin.at[0, pl.ds(1, PLANE - 1)] if dz == 0 else fin.at[dz]
        remote(part, part, fss, grs.at[dz], here).wait_recv()

    rows = PLANE * OWN
    wait_group(0)
    shift = jnp.zeros((OWN, HALF), F32)
    for i in range(PLANE):
        shift += fin[0, i].astype(F32)
    shift = jnp.sum(shift, axis=0, keepdims=True) * (1.0 / rows)

    def add_group(dz, carry):
        def one(i, carry):
            total, square = carry
            d = fin[dz, i].astype(F32) - shift
            return total + d, square + d * d

        return lax.fori_loop(0, PLANE, one, carry, unroll=4)

    zero = jnp.zeros((OWN, HALF), F32)
    carry = add_group(0, (zero, zero))
    late = ()
    for pair in PAIRS:
        for kx in KX:
            for dz in pair:
                wait_z(dz, kx)
                forward(dz, kx)
        for dz in late:
            wait_group(dz)
            carry = add_group(dz, carry)
        late = pair
    for dz in late:
        wait_group(dz)
        carry = add_group(dz, carry)

    first = jnp.sum(carry[0], axis=0, keepdims=True) * (1.0 / SAMPLES)
    second = jnp.sum(carry[1], axis=0, keepdims=True) * (1.0 / SAMPLES)
    mean = shift + first
    var = second - first * first
    live = counts[assign[me]]
    column = lax.broadcasted_iota(jnp.int32, (1, HALF), 1) + row * HALF
    mask = jnp.where(column < live, 1.0, 0.0)
    scale = lax.rsqrt(var + EPS) * mask

    copies = []
    groups = CHUNK // rows
    for c in range(SAMPLES // CHUNK):
        part = fin[pl.ds(c * groups, groups)].reshape(CHUNK, HALF)
        part = ((part.astype(F32) - mean) * scale).astype(BF)
        std[c] = part
        both = nt(bsplit[...], part)
        pbuf[c] = both[:RANK] + both[RANK:]
        copy = remote(pbuf.at[c], precv.at[c], pss.at[c], prs.at[c], mate)
        copy.start()
        copies.append(copy)
    acc = jnp.zeros((2 * RANK, HALF), F32)
    for c in range(SAMPLES // CHUNK):
        copies[c].wait_recv()
        acc += nn(split(pbuf[c] + precv[c]), std[c])
    product = acc[:RANK] + acc[RANK:]
    image = product * (SHRINK / SAMPLES) + (1.0 - SHRINK) * (basis[...] * mask)
    image_out[...] = image
    halves = split(image)
    outer = nt(halves, halves[:RANK]) + nt(halves, halves[RANK:])
    gbuf[:, pl.ds(0, RANK)] = outer[:RANK] + outer[RANK:]
    swap = remote(gbuf, grecv, gss, grr, mate)
    swap.start()
    for copy in copies:
        copy.wait_send()
    for dz in range(NZ):
        part = fin.at[dz, pl.ds(1, PLANE - 1)]
        remote(part, part, fss, grs.at[dz], here).wait_send()
    part = send.at[pl.ds(0, (NZ - 1) * PLANE)]
    remote(part, part, zss, grs.at[0], here).wait_send()
    swap.wait_recv()
    gram_out[...] = gbuf[...] + grecv[...]
    swap.wait_send()


def spread(row, n):
    return jnp.broadcast_to(row, (n, row.shape[1]))


def factor_kernel(image_in, gram, image_out, basis_out, factor_out):
    wide = 2 * RANK
    image = image_in[...]
    image_out[...] = image
    lane = lax.broadcasted_iota(jnp.int32, (RANK, wide), 1)
    line = lax.broadcasted_iota(jnp.int32, (RANK, wide), 0)
    work = jnp.where(lane < RANK, gram[...], jnp.where(lane == line + RANK, 1.0, 0.0))
    tiles = [work[8 * b : 8 * b + 8] for b in range(8)]
    below = lax.broadcasted_iota(jnp.int32, (8, wide), 0)
    done = []
    for p in range(8):
        cols = {
            (c, b): jnp.broadcast_to(tiles[b][:, 8 * p + c : 8 * p + c + 1], (8, wide))
            for c in range(8)
            for b in range(p, 8)
        }
        finished = jnp.zeros((8, wide), F32)
        for c in range(8):
            inv = lax.rsqrt(spread(cols[c, p][c : c + 1], 8))
            line_c = spread(tiles[p][c : c + 1], 8) * inv
            finished = jnp.where(below == c, line_c, finished)
            lows = [cols[c, b] * inv for b in range(p, 8)]
            for d in range(c + 1, 8):
                factor = spread(lows[0][d : d + 1], 8)
                for b in range(p, 8):
                    cols[d, b] = cols[d, b] - lows[b - p] * factor
            for b in range(p, 8):
                tiles[b] = tiles[b] - lows[b - p] * line_c
        done.append(finished)
    full = jnp.concatenate(done, axis=0)
    upper = jnp.where((lane < RANK) & (lane >= line), full, 0.0)
    factor_out[...] = jnp.transpose(upper[:, :RANK])
    inverse = jnp.where((lane >= RANK) & (lane - RANK <= line), full, 0.0)
    both = split(inverse)
    halves = split(image)
    high = jnp.concatenate([halves[:RANK], halves[:RANK]], axis=0)
    low = jnp.concatenate([halves[RANK:], halves[RANK:]], axis=0)
    one = nn(both, high)
    two = nn(both[:RANK], low)
    basis_out[...] = one[:RANK] + one[RANK:] + two


def body(genotypes, assignment, snp_counts, basis):
    vmem = pl.BlockSpec(memory_space=pltpu.VMEM)
    smem = pl.BlockSpec(memory_space=pltpu.SMEM)
    dma = pltpu.SemaphoreType.DMA
    chunks = SAMPLES // CHUNK
    image, gram = pl.pallas_call(
        exchange_kernel,
        out_shape=(
            jax.ShapeDtypeStruct((RANK, HALF), F32),
            jax.ShapeDtypeStruct((RANK, 2 * RANK), F32),
        ),
        in_specs=[smem, smem, vmem, vmem],
        out_specs=(vmem, vmem),
        scratch_shapes=[
            pltpu.VMEM((PLANE * OWN, SAMPLES), BF),
            pltpu.VMEM((BLOCKS, OWN, HALF), BF),
            pltpu.VMEM((NZ, NX, NY, OWN, HALF), BF),
            pltpu.VMEM((NZ, PLANE, OWN, HALF), BF),
            pltpu.VMEM((chunks, CHUNK, HALF), BF),
            pltpu.VMEM((2 * RANK, HALF), BF),
            pltpu.VMEM((chunks, RANK, CHUNK), F32),
            pltpu.VMEM((chunks, RANK, CHUNK), F32),
            pltpu.VMEM((RANK, 2 * RANK), F32),
            pltpu.VMEM((RANK, 2 * RANK), F32),
            dma, dma, dma((chunks,)), dma,
            dma((NZ, NX)), dma((NZ,)), dma((chunks,)), dma,
        ],
        compiler_params=pltpu.CompilerParams(
            collective_id=0, has_side_effects=True, vmem_limit_bytes=32 << 20
        ),
        name="exchange",
    )(assignment, snp_counts, genotypes, basis.reshape(RANK, HALF))
    image, new_basis, factor = pl.pallas_call(
        factor_kernel,
        out_shape=(
            jax.ShapeDtypeStruct((RANK, HALF), F32),
            jax.ShapeDtypeStruct((RANK, HALF), F32),
            jax.ShapeDtypeStruct((RANK, RANK), F32),
        ),
        in_specs=[vmem, vmem],
        out_specs=(vmem, vmem, vmem),
        compiler_params=pltpu.CompilerParams(vmem_limit_bytes=8 << 20),
        name="factorize",
    )(image, gram)
    return image[None], new_basis[None], factor[None]


def solution(mesh):
    in_specs = (P("blk", None, "row"), P(), P(), P("blk", None, "row"))
    out_specs = (P("blk", None, "row"), P("blk", None, "row"), P("blk", None, None))
    return jax.shard_map(body, mesh=mesh, in_specs=in_specs, out_specs=out_specs, check_vma=False)
```

```python
import functools

import jax
import jax.numpy as jnp
from jax import lax
from jax.experimental import pallas as pl
from jax.experimental.pallas import tpu as pltpu
from jax.sharding import PartitionSpec as P

EPS = 1e-05
SHRINK = 0.5
MESH = pl.DeviceIdType.MESH
NX, NZ, NY = 4, 8, 4
PLANE = NX * NY
BLOCKS = NX * NZ * NY
OWN = 8
SAMPLES = BLOCKS * OWN
HALF = 1024
RANK = 64
CHUNK = 256
KX = (1, 2, 3, 0)
ORDER = (4, 3, 5, 2, 6, 1, 7, 0)
BF = jnp.bfloat16
F32 = jnp.float32


def block_of(x, z, y):
    return (x * NZ + z) * NY + y


def remote(src, dst, send_sem, recv_sem, to):
    return pltpu.make_async_remote_copy(
        src_ref=src, dst_ref=dst, send_sem=send_sem, recv_sem=recv_sem,
        device_id=to, device_id_type=MESH,
    )


def split(value):
    high = value.astype(BF)
    low = (value - high.astype(F32)).astype(BF)
    return jnp.concatenate([high, low], axis=0)


def nt(a, b):
    return lax.dot_general(a, b, (((1,), (1,)), ((), ())), preferred_element_type=F32)


def nn(a, b):
    return lax.dot_general(a, b, (((1,), (0,)), ((), ())), preferred_element_type=F32)


def exchange_kernel(
    assign_in, counts_in, geno_in, basis_in, image_out, gram_out,
    assign, counts, geno, basis, pick, send, zbuf, fin, std, bsplit, pbuf, precv, gbuf, grecv,
    load_sem, zss, fss, pss, gss, zrs, grs, prs, grr,
):
    me = lax.axis_index("blk")
    row = lax.axis_index("row")
    y = me % NY
    z = (me // NY) % NZ
    x = me // (NY * NZ)
    mate = {"row": 1 - row}
    here = {"blk": me}

    loads = [
        pltpu.make_async_copy(src, dst, load_sem.at[i])
        for i, (src, dst) in enumerate(
            ((assign_in, assign), (geno_in, geno), (basis_in, basis), (counts_in, counts))
        )
    ]
    for load in loads:
        load.start()
    barrier = pltpu.get_barrier_semaphore()
    xs = [(x + k) % NX for k in range(NX)]
    ys = [(y + k) % NY for k in range(NY)]
    peers = [{"blk": block_of(x, (z + d) % NZ, y)} for d in range(1, NZ)]
    peers += [
        {"blk": block_of(xs[i], z, ys[j])} for i in range(NX) for j in range(NY) if i or j
    ]
    peers.append(mate)
    for peer in peers:
        pl.semaphore_signal(barrier, inc=1, device_id=peer, device_id_type=MESH)

    gbuf[...] = jnp.zeros_like(gbuf)
    offset = (
        lax.broadcasted_iota(jnp.int32, (OWN, SAMPLES), 1)
        - BLOCKS * lax.broadcasted_iota(jnp.int32, (OWN, SAMPLES), 0)
    )

    loads[0].wait()

    def permute(kx, half):
        column = (x + kx) % NX
        planes = []
        for i in range(4):
            dz = jnp.where(half == 0, ORDER[i], ORDER[4 + i])
            planes.append((dz, (z + dz) % NZ))
        for i, (_, zt) in enumerate(planes):
            for j in range(NY):
                slot = block_of(column, zt, j)
                pick[pl.ds((i * NY + j) * OWN, OWN), :] = jnp.where(
                    offset == assign[slot], 1.0, 0.0
                ).astype(BF)
        table = geno[...].reshape(SAMPLES, HALF)
        moved = nn(pick[...], table).astype(BF).reshape(4, NY, OWN, HALF)
        for i, (_, zt) in enumerate(planes):
            send[pl.ds(block_of(column, zt, 0), NY)] = moved[i]
        return column, planes

    def forward(dz, kx, column, src):
        def one(ky):
            yt = ys[ky]
            to = block_of(column, z, yt)
            remote(src(to, yt), fin.at[kx * NY + ky, dz], fss, grs.at[kx], {"blk": to}).start()

        for ky in range(1, NY):
            one(ky)
        if isinstance(kx, int):
            if kx:
                one(0)
        else:
            pl.when(kx > 0)(lambda: one(0))

    def from_send(to, yt):
        return send.at[to]

    def push(i, _):
        kx, half = (i // 2 + 1) % NX, i % 2
        pl.when(i == 0)(loads[1].wait)
        column, planes = permute(kx, half)
        pl.when(i == 0)(lambda: pl.semaphore_wait(barrier, len(peers)))
        for j, (dz, zt) in enumerate(planes):
            to = {"blk": block_of(x, zt, y)}

            def whole():
                remote(
                    send.at[pl.ds(block_of(column, zt, 0), NY)], zbuf.at[dz, kx],
                    zss, zrs.at[dz, kx], to,
                ).start()

            def three():
                for ky in range(1, NY):
                    remote(
                        send.at[block_of(x, zt, ys[ky])], zbuf.at[dz, 0, ys[ky]],
                        zss, zrs.at[dz, 0], to,
                    ).start()

            def either():
                pl.when(kx > 0)(whole)
                pl.when(kx == 0)(three)

            if j < 3:
                either()
            else:
                pl.when(half == 0)(either)
                pl.when(half == 1)(lambda: forward(0, kx, column, from_send))
        return 0

    lax.fori_loop(0, 8, push, 0)
    for dz in ORDER[:7]:
        zt = (z + dz) % NZ
        to = block_of(x, zt, y)
        remote(send.at[to], fin.at[0, dz], zss, grs.at[4], {"blk": to}).start()
    fin[0, 0] = send[me]
    loads[2].wait()
    loads[3].wait()
    bsplit[...] = split(basis[...])

    def wait_group(part, sem):
        remote(part, part, fss, grs.at[sem], here).wait_recv()

    def add_rows(first_slot, count, shift, carry):
        def one(i, carry):
            total, square = carry
            d = fin[first_slot + i // NZ, i % NZ].astype(F32) - shift
            return total + d, square + d * d

        return lax.fori_loop(0, count, one, carry, unroll=4)

    zero = jnp.zeros((OWN, HALF), F32)
    shift, carry = None, (zero, zero)
    for step, kx in enumerate(KX):
        for dz in ORDER[:7]:
            part = zbuf.at[dz, 0, pl.ds(0, 3)] if kx == 0 else zbuf.at[dz, 0]
            remote(part, part, zss, zrs.at[dz, kx], here).wait_recv()
            forward(dz, kx, xs[kx], lambda to, yt: zbuf.at[dz, kx, yt])
        if step == 0:
            continue
        prev = KX[step - 1]
        wait_group(fin.at[pl.ds(prev * NY, NY)], prev)
        if step == 1:
            rows = NY * NZ

            def one(i, total):
                return total + fin[NY + i // NZ, i % NZ].astype(F32)

            shift = lax.fori_loop(0, rows, one, zero, unroll=4)
            shift = jnp.sum(shift, axis=0, keepdims=True) * (1.0 / (rows * OWN))
        carry = add_rows(prev * NY, NY * NZ, shift, carry)
    wait_group(fin.at[pl.ds(1, NY - 1)], 0)
    carry = add_rows(1, (NY - 1) * NZ, shift, carry)
    wait_group(fin.at[0, pl.ds(1, NZ - 1)], 4)
    carry = add_rows(0, NZ, shift, carry)

    first = jnp.sum(carry[0], axis=0, keepdims=True) * (1.0 / SAMPLES)
    second = jnp.sum(carry[1], axis=0, keepdims=True) * (1.0 / SAMPLES)
    mean = shift + first
    var = second - first * first
    live = counts[assign[me]]
    column = lax.broadcasted_iota(jnp.int32, (1, HALF), 1) + row * HALF
    mask = jnp.where(column < live, 1.0, 0.0)
    scale = lax.rsqrt(var + EPS) * mask

    copies = {}
    for c in KX:
        part = fin[pl.ds(c * NY, NY)].reshape(CHUNK, HALF)
        part = ((part.astype(F32) - mean) * scale).astype(BF)
        std[c] = part
        both = nt(bsplit[...], part)
        pbuf[c] = both[:RANK] + both[RANK:]
        copies[c] = remote(pbuf.at[c], precv.at[c], pss.at[c], prs.at[c], mate)
        copies[c].start()
    acc = jnp.zeros((2 * RANK, HALF), F32)
    for c in KX:
        copies[c].wait_recv()
        acc += nn(split(pbuf[c] + precv[c]), std[c])
    product = acc[:RANK] + acc[RANK:]
    image = product * (SHRINK / SAMPLES) + (1.0 - SHRINK) * (basis[...] * mask)
    image_out[...] = image
    halves = split(image)
    outer = nt(halves, halves[:RANK]) + nt(halves, halves[RANK:])
    gbuf[:, pl.ds(0, RANK)] = outer[:RANK] + outer[RANK:]
    swap = remote(gbuf, grecv, gss, grr, mate)
    swap.start()
    for c in KX:
        copies[c].wait_send()
    for dz in range(NZ):
        part = fin.at[pl.ds(1, PLANE - 1), dz]
        remote(part, part, fss, grs.at[0], here).wait_send()
    part = send.at[pl.ds(0, (NZ - 1) * PLANE)]
    remote(part, part, zss, grs.at[0], here).wait_send()
    swap.wait_recv()
    gram_out[...] = gbuf[...] + grecv[...]
    swap.wait_send()


def spread(row, n):
    return jnp.broadcast_to(row, (n, row.shape[1]))


def factor_kernel(image_in, gram, image_out, basis_out, factor_out):
    wide = 2 * RANK
    image = image_in[...]
    image_out[...] = image
    lane = lax.broadcasted_iota(jnp.int32, (RANK, wide), 1)
    line = lax.broadcasted_iota(jnp.int32, (RANK, wide), 0)
    work = jnp.where(lane < RANK, gram[...], jnp.where(lane == line + RANK, 1.0, 0.0))
    tiles = [work[8 * b : 8 * b + 8] for b in range(8)]
    below = lax.broadcasted_iota(jnp.int32, (8, wide), 0)
    done = []
    for p in range(8):
        cols = {
            (c, b): jnp.broadcast_to(tiles[b][:, 8 * p + c : 8 * p + c + 1], (8, wide))
            for c in range(8)
            for b in range(p, 8)
        }
        finished = jnp.zeros((8, wide), F32)
        for c in range(8):
            inv = lax.rsqrt(spread(cols[c, p][c : c + 1], 8))
            line_c = spread(tiles[p][c : c + 1], 8) * inv
            finished = jnp.where(below == c, line_c, finished)
            lows = [cols[c, b] * inv for b in range(p, 8)]
            for d in range(c + 1, 8):
                factor = spread(lows[0][d : d + 1], 8)
                for b in range(p, 8):
                    cols[d, b] = cols[d, b] - lows[b - p] * factor
            for b in range(p, 8):
                tiles[b] = tiles[b] - lows[b - p] * line_c
        done.append(finished)
    full = jnp.concatenate(done, axis=0)
    upper = jnp.where((lane < RANK) & (lane >= line), full, 0.0)
    factor_out[...] = jnp.transpose(upper[:, :RANK])
    inverse = jnp.where((lane >= RANK) & (lane - RANK <= line), full, 0.0)
    both = split(inverse)
    halves = split(image)
    high = jnp.concatenate([halves[:RANK], halves[:RANK]], axis=0)
    low = jnp.concatenate([halves[RANK:], halves[RANK:]], axis=0)
    one = nn(both, high)
    two = nn(both[:RANK], low)
    basis_out[...] = one[:RANK] + one[RANK:] + two


def body(genotypes, assignment, snp_counts, basis):
    vmem = pl.BlockSpec(memory_space=pltpu.VMEM)
    hbm = pl.BlockSpec(memory_space=pltpu.HBM)
    dma = pltpu.SemaphoreType.DMA
    chunks = SAMPLES // CHUNK
    image, gram = pl.pallas_call(
        exchange_kernel,
        out_shape=(
            jax.ShapeDtypeStruct((RANK, HALF), F32),
            jax.ShapeDtypeStruct((RANK, 2 * RANK), F32),
        ),
        in_specs=[hbm] * 4,
        out_specs=(vmem, vmem),
        scratch_shapes=[
            pltpu.SMEM((BLOCKS,), jnp.int32),
            pltpu.SMEM((BLOCKS,), jnp.int32),
            pltpu.VMEM((OWN, BLOCKS, HALF), BF),
            pltpu.VMEM((RANK, HALF), F32),
            pltpu.VMEM((PLANE * OWN, SAMPLES), BF),
            pltpu.VMEM((BLOCKS, OWN, HALF), BF),
            pltpu.VMEM((NZ, NX, NY, OWN, HALF), BF),
            pltpu.VMEM((PLANE, NZ, OWN, HALF), BF),
            pltpu.VMEM((chunks, CHUNK, HALF), BF),
            pltpu.VMEM((2 * RANK, HALF), BF),
            pltpu.VMEM((chunks, RANK, CHUNK), F32),
            pltpu.VMEM((chunks, RANK, CHUNK), F32),
            pltpu.VMEM((RANK, 2 * RANK), F32),
            pltpu.VMEM((RANK, 2 * RANK), F32),
            dma((4,)), dma, dma, dma((chunks,)), dma,
            dma((NZ, NX)), dma((5,)), dma((chunks,)), dma,
        ],
        compiler_params=pltpu.CompilerParams(
            collective_id=0, has_side_effects=True, vmem_limit_bytes=32 << 20
        ),
        name="exchange",
    )(*(
        pltpu.with_memory_space_constraint(a, pltpu.HBM)
        for a in (assignment, snp_counts, genotypes, basis.reshape(RANK, HALF))
    ))
    image, new_basis, factor = pl.pallas_call(
        factor_kernel,
        out_shape=(
            jax.ShapeDtypeStruct((RANK, HALF), F32),
            jax.ShapeDtypeStruct((RANK, HALF), F32),
            jax.ShapeDtypeStruct((RANK, RANK), F32),
        ),
        in_specs=[vmem, vmem],
        out_specs=(vmem, vmem, vmem),
        compiler_params=pltpu.CompilerParams(vmem_limit_bytes=8 << 20),
        name="factorize",
    )(image, gram)
    return image[None], new_basis[None], factor[None]


def solution(mesh):
    in_specs = (P("blk", None, "row"), P(), P(), P("blk", None, "row"))
    out_specs = (P("blk", None, "row"), P("blk", None, "row"), P("blk", None, None))
    return jax.shard_map(body, mesh=mesh, in_specs=in_specs, out_specs=out_specs, check_vma=False)
```

```python
import functools

import jax
import jax.numpy as jnp
from jax import lax
from jax.experimental import pallas as pl
from jax.experimental.pallas import tpu as pltpu
from jax.sharding import PartitionSpec as P

EPS = 1e-05
SHRINK = 0.5
MESH = pl.DeviceIdType.MESH
NX, NZ, NY = 4, 8, 4
PLANE = NX * NY
BLOCKS = NX * NZ * NY
OWN = 8
SAMPLES = BLOCKS * OWN
HALF = 1024
RANK = 64
CHUNK = 256
KX = (1, 2, 3, 0)
ORDER = (4, 3, 5, 2, 6, 1, 7, 0)
BF = jnp.bfloat16
F32 = jnp.float32


def block_of(x, z, y):
    return (x * NZ + z) * NY + y


def remote(src, dst, send_sem, recv_sem, to):
    return pltpu.make_async_remote_copy(
        src_ref=src, dst_ref=dst, send_sem=send_sem, recv_sem=recv_sem,
        device_id=to, device_id_type=MESH,
    )


def split(value):
    high = value.astype(BF)
    low = (value - high.astype(F32)).astype(BF)
    return jnp.concatenate([high, low], axis=0)


def nt(a, b):
    return lax.dot_general(a, b, (((1,), (1,)), ((), ())), preferred_element_type=F32)


def nn(a, b):
    return lax.dot_general(a, b, (((1,), (0,)), ((), ())), preferred_element_type=F32)


def exchange_kernel(
    assign_in, counts_in, geno_in, basis_in, image_out, gram_out,
    assign, counts, geno, basis, pick, send, zbuf, fin, std, bsplit, pbuf, precv, gbuf, grecv,
    load_sem, zss, fss, pss, gss, zrs, grs, prs, grr,
):
    me = lax.axis_index("blk")
    row = lax.axis_index("row")
    y = me % NY
    z = (me // NY) % NZ
    x = me // (NY * NZ)
    mate = {"row": 1 - row}
    here = {"blk": me}

    loads = [
        pltpu.make_async_copy(src, dst, load_sem.at[i])
        for i, (src, dst) in enumerate(
            ((assign_in, assign), (geno_in, geno), (basis_in, basis), (counts_in, counts))
        )
    ]
    for load in loads:
        load.start()
    barrier = pltpu.get_barrier_semaphore()
    xs = [(x + k) % NX for k in range(NX)]
    ys = [(y + k) % NY for k in range(NY)]
    peers = [{"blk": block_of(x, (z + d) % NZ, y)} for d in range(1, NZ)]
    peers += [
        {"blk": block_of(xs[i], z, ys[j])} for i in range(NX) for j in range(NY) if i or j
    ]
    peers.append(mate)
    for peer in peers:
        pl.semaphore_signal(barrier, inc=1, device_id=peer, device_id_type=MESH)

    gbuf[...] = jnp.zeros_like(gbuf)
    offset = (
        lax.broadcasted_iota(jnp.int32, (OWN, SAMPLES), 1)
        - BLOCKS * lax.broadcasted_iota(jnp.int32, (OWN, SAMPLES), 0)
    )

    loads[0].wait()

    def permute(kx, half):
        column = (x + kx) % NX
        planes = []
        for i in range(4):
            dz = jnp.where(half == 0, ORDER[i], ORDER[4 + i])
            planes.append((dz, (z + dz) % NZ))
        for i, (_, zt) in enumerate(planes):
            for j in range(NY):
                slot = block_of(column, zt, j)
                pick[pl.ds((i * NY + j) * OWN, OWN), :] = jnp.where(
                    offset == assign[slot], 1.0, 0.0
                ).astype(BF)
        table = geno[...].reshape(SAMPLES, HALF)
        moved = nn(pick[...], table).astype(BF).reshape(4, NY, OWN, HALF)
        for i, (_, zt) in enumerate(planes):
            send[pl.ds(block_of(column, zt, 0), NY)] = moved[i]
        return column, planes

    def forward(dz, kx, column, src):
        def one(ky):
            yt = ys[ky]
            to = block_of(column, z, yt)
            remote(src(to, yt), fin.at[kx * NY + ky, dz], fss, grs.at[kx], {"blk": to}).start()

        for ky in range(1, NY):
            one(ky)
        if isinstance(kx, int):
            if kx:
                one(0)
        else:
            pl.when(kx > 0)(lambda: one(0))

    def from_send(to, yt):
        return send.at[to]

    def push(i, _):
        kx, half = (i // 2 + 1) % NX, i % 2
        pl.when(i == 0)(loads[1].wait)
        column, planes = permute(kx, half)
        pl.when(i == 0)(lambda: pl.semaphore_wait(barrier, len(peers)))
        for j, (dz, zt) in enumerate(planes):
            to = {"blk": block_of(x, zt, y)}

            def whole():
                remote(
                    send.at[pl.ds(block_of(column, zt, 0), NY)], zbuf.at[dz, kx],
                    zss, zrs.at[dz, kx], to,
                ).start()

            def three():
                for ky in range(1, NY):
                    remote(
                        send.at[block_of(x, zt, ys[ky])], zbuf.at[dz, 0, ys[ky]],
                        zss, zrs.at[dz, 0], to,
                    ).start()

            def either():
                pl.when(kx > 0)(whole)
                pl.when(kx == 0)(three)

            if j < 3:
                either()
            else:
                pl.when(half == 0)(either)
                pl.when(half == 1)(lambda: forward(0, kx, column, from_send))
        return 0

    lax.fori_loop(0, 8, push, 0)
    for dz in ORDER[:7]:
        zt = (z + dz) % NZ
        to = block_of(x, zt, y)
        remote(send.at[to], fin.at[0, dz], zss, grs.at[4], {"blk": to}).start()
    fin[0, 0] = send[me]
    loads[2].wait()
    loads[3].wait()
    bsplit[...] = split(basis[...])

    def wait_group(part, sem):
        remote(part, part, fss, grs.at[sem], here).wait_recv()

    def add_rows(first_slot, count, shift, carry):
        def one(i, carry):
            total, square = carry
            d = fin[first_slot + i // NZ, i % NZ].astype(F32) - shift
            return total + d, square + d * d

        return lax.fori_loop(0, count, one, carry, unroll=4)

    zero = jnp.zeros((OWN, HALF), F32)
    shift, carry = None, (zero, zero)
    for step, kx in enumerate(KX):
        for dz in ORDER[:7]:
            part = zbuf.at[dz, 0, pl.ds(0, 3)] if kx == 0 else zbuf.at[dz, 0]
            remote(part, part, zss, zrs.at[dz, kx], here).wait_recv()
            forward(dz, kx, xs[kx], lambda to, yt: zbuf.at[dz, kx, yt])
        if step == 0:
            continue
        prev = KX[step - 1]
        wait_group(fin.at[pl.ds(prev * NY, NY)], prev)
        if step == 1:
            rows = NY * NZ

            def one(i, total):
                return total + fin[NY + i // NZ, i % NZ].astype(F32)

            shift = lax.fori_loop(0, rows, one, zero, unroll=4)
            shift = jnp.sum(shift, axis=0, keepdims=True) * (1.0 / (rows * OWN))
        carry = add_rows(prev * NY, NY * NZ, shift, carry)
    wait_group(fin.at[pl.ds(1, NY - 1)], 0)
    carry = add_rows(1, (NY - 1) * NZ, shift, carry)
    wait_group(fin.at[0, pl.ds(1, NZ - 1)], 4)
    carry = add_rows(0, NZ, shift, carry)

    first = jnp.sum(carry[0], axis=0, keepdims=True) * (1.0 / SAMPLES)
    second = jnp.sum(carry[1], axis=0, keepdims=True) * (1.0 / SAMPLES)
    mean = shift + first
    var = second - first * first
    live = counts[assign[me]]
    column = lax.broadcasted_iota(jnp.int32, (1, HALF), 1) + row * HALF
    mask = jnp.where(column < live, 1.0, 0.0)
    scale = lax.rsqrt(var + EPS) * mask

    copies = {}
    for c in KX:
        part = fin[pl.ds(c * NY, NY)].reshape(CHUNK, HALF)
        part = ((part.astype(F32) - mean) * scale).astype(BF)
        std[c] = part
        both = nt(bsplit[...], part)
        pbuf[c] = both[:RANK] + both[RANK:]
        copies[c] = remote(pbuf.at[c], precv.at[c], pss.at[c], prs.at[c], mate)
        copies[c].start()
    acc = jnp.zeros((2 * RANK, HALF), F32)
    for c in KX:
        copies[c].wait_recv()
        acc += nn(split(pbuf[c] + precv[c]), std[c])
    product = acc[:RANK] + acc[RANK:]
    image = product * (SHRINK / SAMPLES) + (1.0 - SHRINK) * (basis[...] * mask)
    image_out[...] = image
    halves = split(image)
    outer = nt(halves, halves[:RANK]) + nt(halves, halves[RANK:])
    gbuf[:, pl.ds(0, RANK)] = outer[:RANK] + outer[RANK:]
    swap = remote(gbuf, grecv, gss, grr, mate)
    swap.start()
    for c in KX:
        copies[c].wait_send()
    for dz in range(NZ):
        part = fin.at[pl.ds(1, PLANE - 1), dz]
        remote(part, part, fss, grs.at[0], here).wait_send()
    part = send.at[pl.ds(0, (NZ - 1) * PLANE)]
    remote(part, part, zss, grs.at[0], here).wait_send()
    swap.wait_recv()
    gram_out[...] = gbuf[...] + grecv[...]
    swap.wait_send()


def spread(row, n):
    return jnp.broadcast_to(row, (n, row.shape[1]))


def factor_kernel(image_in, gram, image_out, basis_out, factor_out, sem):
    wide = 2 * RANK
    image = image_in[...]
    copy = pltpu.make_async_copy(image_in, image_out, sem)
    copy.start()
    lane = lax.broadcasted_iota(jnp.int32, (RANK, wide), 1)
    line = lax.broadcasted_iota(jnp.int32, (RANK, wide), 0)
    work = jnp.where(lane < RANK, gram[...], jnp.where(lane == line + RANK, 1.0, 0.0))
    tiles = [work[8 * b : 8 * b + 8] for b in range(8)]
    below = lax.broadcasted_iota(jnp.int32, (8, wide), 0)
    done = []
    for p in range(8):
        cols = {
            (c, b): jnp.broadcast_to(tiles[b][:, 8 * p + c : 8 * p + c + 1], (8, wide))
            for c in range(8)
            for b in range(p, 8)
        }
        finished = jnp.zeros((8, wide), F32)
        for c in range(8):
            inv = lax.rsqrt(spread(cols[c, p][c : c + 1], 8))
            line_c = spread(tiles[p][c : c + 1], 8) * inv
            finished = jnp.where(below == c, line_c, finished)
            lows = [cols[c, b] * inv for b in range(p, 8)]
            for d in range(c + 1, 8):
                factor = spread(lows[0][d : d + 1], 8)
                for b in range(p, 8):
                    cols[d, b] = cols[d, b] - lows[b - p] * factor
            for b in range(p, 8):
                tiles[b] = tiles[b] - lows[b - p] * line_c
        done.append(finished)
    full = jnp.concatenate(done, axis=0)
    upper = jnp.where((lane < RANK) & (lane >= line), full, 0.0)
    factor_out[...] = jnp.transpose(upper[:, :RANK])
    inverse = jnp.where((lane >= RANK) & (lane - RANK <= line), full, 0.0)
    both = split(inverse)
    halves = split(image)
    high = jnp.concatenate([halves[:RANK], halves[:RANK]], axis=0)
    low = jnp.concatenate([halves[RANK:], halves[RANK:]], axis=0)
    one = nn(both, high)
    two = nn(both[:RANK], low)
    basis_out[...] = one[:RANK] + one[RANK:] + two
    copy.wait()


def body(genotypes, assignment, snp_counts, basis):
    vmem = pl.BlockSpec(memory_space=pltpu.VMEM)
    hbm = pl.BlockSpec(memory_space=pltpu.HBM)
    dma = pltpu.SemaphoreType.DMA
    chunks = SAMPLES // CHUNK
    image, gram = pl.pallas_call(
        exchange_kernel,
        out_shape=(
            jax.ShapeDtypeStruct((RANK, HALF), F32),
            jax.ShapeDtypeStruct((RANK, 2 * RANK), F32),
        ),
        in_specs=[hbm] * 4,
        out_specs=(vmem, vmem),
        scratch_shapes=[
            pltpu.SMEM((BLOCKS,), jnp.int32),
            pltpu.SMEM((BLOCKS,), jnp.int32),
            pltpu.VMEM((OWN, BLOCKS, HALF), BF),
            pltpu.VMEM((RANK, HALF), F32),
            pltpu.VMEM((PLANE * OWN, SAMPLES), BF),
            pltpu.VMEM((BLOCKS, OWN, HALF), BF),
            pltpu.VMEM((NZ, NX, NY, OWN, HALF), BF),
            pltpu.VMEM((PLANE, NZ, OWN, HALF), BF),
            pltpu.VMEM((chunks, CHUNK, HALF), BF),
            pltpu.VMEM((2 * RANK, HALF), BF),
            pltpu.VMEM((chunks, RANK, CHUNK), F32),
            pltpu.VMEM((chunks, RANK, CHUNK), F32),
            pltpu.VMEM((RANK, 2 * RANK), F32),
            pltpu.VMEM((RANK, 2 * RANK), F32),
            dma((4,)), dma, dma, dma((chunks,)), dma,
            dma((NZ, NX)), dma((5,)), dma((chunks,)), dma,
        ],
        compiler_params=pltpu.CompilerParams(
            collective_id=0, has_side_effects=True, vmem_limit_bytes=32 << 20
        ),
        name="exchange",
    )(*(
        pltpu.with_memory_space_constraint(a, pltpu.HBM)
        for a in (assignment, snp_counts, genotypes, basis.reshape(RANK, HALF))
    ))
    image, new_basis, factor = pl.pallas_call(
        factor_kernel,
        out_shape=(
            jax.ShapeDtypeStruct((RANK, HALF), F32),
            jax.ShapeDtypeStruct((RANK, HALF), F32),
            jax.ShapeDtypeStruct((RANK, RANK), F32),
        ),
        in_specs=[vmem, vmem],
        out_specs=(hbm, vmem, vmem),
        scratch_shapes=[dma],
        compiler_params=pltpu.CompilerParams(vmem_limit_bytes=8 << 20),
        name="factorize",
    )(image, gram)
    return image[None], new_basis[None], factor[None]


def solution(mesh):
    in_specs = (P("blk", None, "row"), P(), P(), P("blk", None, "row"))
    out_specs = (P("blk", None, "row"), P("blk", None, "row"), P("blk", None, None))
    return jax.shard_map(body, mesh=mesh, in_specs=in_specs, out_specs=out_specs, check_vma=False)
```
